32 devices in a mesh: dp: 4 (over z), fsdp: 8 (over y, x, core).
Axes of the slice: x: 2, y: 2, z: 4, core: 2. Of those that a mesh axis runs over, the one named last changes fastest.
Arguments:
- tokens: bfloat16 [4096, 1536], P(('dp', 'fsdp')), may hold values from -6 to 6
- segments: int32 [32, 128], P(('dp', 'fsdp')), may hold values from 0 to 3, never falling along the last dimension, each value on 1 to 64 neighbouring positions
- cotangent: bfloat16 [4096, 1536], P(('dp', 'fsdp')), may hold values from -6 to 6
- norm_gains: bfloat16 [2, 1536], P(None, ('dp', 'fsdp')), may hold values from 0.5 to 1.5
- w_query: bfloat16 [1536, 1536], P(('dp', 'fsdp')), may hold values from -0.15625 to 0.15625
- w_key: bfloat16 [1536, 768], P(('dp', 'fsdp')), may hold values from -0.15625 to 0.15625
- w_value: bfloat16 [1536, 768], P(('dp', 'fsdp')), may hold values from -0.15625 to 0.15625
- w_out: bfloat16 [1536, 1536], P(('dp', 'fsdp')), may hold values from -0.875 to 0.875
- w_gate: bfloat16 [1536, 4096], P(('dp', 'fsdp')), may hold values from -0.15625 to 0.15625
- w_up: bfloat16 [1536, 4096], P(('dp', 'fsdp')), may hold values from -0.15625 to 0.15625
- w_down: bfloat16 [4096, 1536], P(('dp', 'fsdp')), may hold values from -0.09375 to 0.09375
- moment_gains: float32 [2, 1536], P(None, ('dp', 'fsdp')), may hold values from -128 to 128
- moment_query: float32 [1536, 1536], P(('dp', 'fsdp')), may hold values from -128 to 128
- moment_key: float32 [1536, 768], P(('dp', 'fsdp')), may hold values from -128 to 128
- moment_value: float32 [1536, 768], P(('dp', 'fsdp')), may hold values from -256 to 256
- moment_out: float32 [1536, 1536], P(('dp', 'fsdp')), may hold values from -32 to 32
- moment_gate: float32 [1536, 4096], P(('dp', 'fsdp')), may hold values from -32 to 32
- moment_up: float32 [1536, 4096], P(('dp', 'fsdp')), may hold values from -32 to 32
- moment_down: float32 [4096, 1536], P(('dp', 'fsdp')), may hold values from -32 to 32
Outputs:
- outputs: bfloat16 [4096, 1536], P(('dp', 'fsdp'))
- grad_tokens: float32 [4096, 1536], P(('dp', 'fsdp'))
- grad_gains: float32 [2, 1536], P(None, ('dp', 'fsdp'))
- grad_query: float32 [1536, 1536], P(('dp', 'fsdp'))
- grad_key: float32 [1536, 768], P(('dp', 'fsdp'))
- grad_value: float32 [1536, 768], P(('dp', 'fsdp'))
- grad_out: float32 [1536, 1536], P(('dp', 'fsdp'))
- grad_gate: float32 [1536, 4096], P(('dp', 'fsdp'))
- grad_up: float32 [1536, 4096], P(('dp', 'fsdp'))
- grad_down: float32 [4096, 1536], P(('dp', 'fsdp'))
- update_gains: float32 [2, 1536], P(None, ('dp', 'fsdp'))
- update_query: float32 [1536, 1536], P(('dp', 'fsdp'))
- update_key: float32 [1536, 768], P(('dp', 'fsdp'))
- update_value: float32 [1536, 768], P(('dp', 'fsdp'))
- update_out: float32 [1536, 1536], P(('dp', 'fsdp'))
- update_gate: float32 [1536, 4096], P(('dp', 'fsdp'))
- update_up: float32 [1536, 4096], P(('dp', 'fsdp'))
- update_down: float32 [4096, 1536], P(('dp', 'fsdp'))
- new_moment_gains: float32 [2, 1536], P(None, ('dp', 'fsdp'))
- new_moment_query: float32 [1536, 1536], P(('dp', 'fsdp'))
- new_moment_key: float32 [1536, 768], P(('dp', 'fsdp'))
- new_moment_value: float32 [1536, 768], P(('dp', 'fsdp'))
- new_moment_out: float32 [1536, 1536], P(('dp', 'fsdp'))
- new_moment_gate: float32 [1536, 4096], P(('dp', 'fsdp'))
- new_moment_up: float32 [1536, 4096], P(('dp', 'fsdp'))
- new_moment_down: float32 [4096, 1536], P(('dp', 'fsdp'))
The draws below stay inside these ranges and needn't reach their ends.
Inputs may be any that keep to these rules, and one draw needn't show every extreme that they name: `segments`: within each sequence the document numbers never fall; each document holds 1 to 64 tokens.
All inputs are finite; a program needn't handle non-finite values.
Results may differ from the reference program's by a relative error of at most 0.025.
Values may be sent and summed in bfloat16 or wider, within the bound.
A program may use at most 320 MiB of HBM per device.

```python
import math
import jax
import jax.numpy as jnp
import numpy as np
from jax import lax

D = 1536
HEADS = 16
KV_HEADS = 8
HEAD_DIM = 96
FF = 4096
SEQ_LEN = 128
NS_STEPS = 3
KVW = 768
NSEQ = 32
TOKENS = 4096


def level_of(key, dims, shards, least, top_value):
    factor_of, own = 1.0, jax.random.fold_in(key, 6)
    for axis_at, shards_of in shards:
        heights = jnp.exp(jax.random.uniform(jax.random.fold_in(own, axis_at), (shards_of,), jnp.float32, least / len(shards), top_value / len(shards)))
        factor_of = factor_of * jnp.repeat(heights, dims[axis_at] // shards_of).reshape([-1 if axis == axis_at else 1 for axis in range(len(dims))])
    return factor_of


def split_up(number_of, total, limit, skew):
    portions = [(1 << 20) // math.isqrt(rank ** skew) + 1 for rank in range(2, number_of + 1)]
    rest, given = total - limit - (number_of - 1), [1] * (number_of - 1)
    while rest > 0:
        candidates = [i for i in range(number_of - 1) if given[i] < limit]
        whole, left = sum([portions[i] for i in candidates]), rest
        for i in candidates:
            more = min(limit - given[i], max(1, left * portions[i] // whole), rest)
            given[i] = given[i] + more
            rest = rest - more
    return np.array([limit] + given)


def ragged(stream_key, count, total, reach, lean):
    if count == 2:
        one = jax.random.randint(stream_key, (), max(1, total - reach), min(reach, total - 1) + 1)
        return jnp.stack([one, total - one])
    tallies = jnp.asarray(split_up(count, total, reach, lean), jnp.int32)
    pairs = (count - 1) // 2
    donor, receiver = tallies[1:1 + 2 * pairs:2], tallies[2:2 + 2 * pairs:2]
    slack = jnp.minimum(donor - 1, reach - receiver)
    shifted = jax.random.randint(jax.random.fold_in(stream_key, 1), (pairs,), 0, 1 << 20) % (slack + 1)
    tallies = tallies.at[1:1 + 2 * pairs:2].set(donor - shifted).at[2:2 + 2 * pairs:2].set(receiver + shifted)
    return tallies[jax.random.permutation(jax.random.fold_in(stream_key, 2), count)]


def bell_draw(rng, dims, scale, reach, shards=(), kind=jnp.bfloat16):
    level = level_of(rng, dims, shards, -0.22, 0.18) if shards else 1.0
    values = jax.random.normal(rng, dims, jnp.float32) * scale * level
    return jnp.minimum(jnp.maximum(values, -reach), reach).astype(kind)


def setup_inputs(seed: int = 0) -> dict:
    streams_of = jax.random.split(jax.random.key(seed), 20)
    tokens = bell_draw(streams_of[0], (TOKENS, D), 1.0, 6.0, ((0, 32),))
    segments = jax.vmap(lambda own: jnp.searchsorted(jnp.cumsum(ragged(own, 4, SEQ_LEN, SEQ_LEN // 2, 2)), jnp.arange(SEQ_LEN), side="right"))(jax.random.split(streams_of[1], NSEQ)).reshape((NSEQ, SEQ_LEN)).astype(jnp.int32)
    cotangent = bell_draw(streams_of[2], (TOKENS, D), 1.0, 6.0, ((0, 32),))
    norm_gains = jnp.clip(1.0 + 0.1 * jax.random.normal(streams_of[3], (2, D), jnp.float32), 0.5, 1.5).astype(jnp.bfloat16)
    w_query = bell_draw(streams_of[4], (D, D), D ** -0.5, 0.15625, ((0, 32),))
    w_key = bell_draw(streams_of[5], (D, KVW), D ** -0.5, 0.15625, ((0, 32),))
    w_value = bell_draw(streams_of[6], (D, KVW), D ** -0.5, 0.15625, ((0, 32),))
    w_out = bell_draw(streams_of[7], (D, D), (D // 32) ** -0.5, 0.875, ((0, 32),))
    w_gate = bell_draw(streams_of[8], (D, FF), D ** -0.5, 0.15625, ((0, 32),))
    w_up = bell_draw(streams_of[9], (D, FF), D ** -0.5, 0.15625, ((0, 32),))
    w_down = bell_draw(streams_of[10], (FF, D), FF ** -0.5, 0.09375, ((0, 32),))
    moment_gains = bell_draw(streams_of[11], (2, D), (4 * (TOKENS // 1024 + 1)), 128.0, ((1, 32),), jnp.float32)
    moment_query = bell_draw(streams_of[12], (D, D), (4 * (TOKENS // 1024 + 1)), 128.0, ((0, 32),), jnp.float32)
    moment_key = bell_draw(streams_of[13], (D, KVW), (4 * (TOKENS // 1024 + 1)), 128.0, ((0, 32),), jnp.float32)
    moment_value = bell_draw(streams_of[14], (D, KVW), (8 * (TOKENS // 1024 + 1)), 256.0, ((0, 32),), jnp.float32)
    moment_out = bell_draw(streams_of[15], (D, D), (TOKENS // 1024 + 1), 32.0, ((0, 32),), jnp.float32)
    moment_gate = bell_draw(streams_of[16], (D, FF), (TOKENS // 1024 + 1), 32.0, ((0, 32),), jnp.float32)
    moment_up = bell_draw(streams_of[17], (D, FF), (TOKENS // 1024 + 1), 32.0, ((0, 32),), jnp.float32)
    moment_down = bell_draw(streams_of[18], (FF, D), (TOKENS // 1024 + 1), 32.0, ((0, 32),), jnp.float32)
    return dict(tokens=tokens, segments=segments, cotangent=cotangent, norm_gains=norm_gains, w_query=w_query, w_key=w_key, w_value=w_value, w_out=w_out, w_gate=w_gate, w_up=w_up, w_down=w_down, moment_gains=moment_gains, moment_query=moment_query, moment_key=moment_key, moment_value=moment_value, moment_out=moment_out, moment_gate=moment_gate, moment_up=moment_up, moment_down=moment_down)


@jax.custom_vjp
def low(v):
    return lax.optimization_barrier(v.astype(jnp.bfloat16)).astype(jnp.float32)

@jax.custom_vjp
def low_back(v):
    return v

def low_keep(v):
    return (low(v), None)

def low_pass(kept, grad):
    return (grad,)

def back_keep(v):
    return (v, None)

def back_low(kept, grad):
    return (low(grad),)
low.defvjp(low_keep, low_pass)
low_back.defvjp(back_keep, back_low)
eps_norm = 1e-05
rope_base = 100000.0
coeff_a = 3.4445
coeff_b = -4.775
coeff_c = 2.0315
beta_moment = 0.95
rate_matrix = 0.2
rate_gain = 0.05
masked_score = -1e+30

def mixed(left_side, right_side):
    return jnp.dot(left_side, right_side, precision=lax.Precision.HIGHEST, preferred_element_type=jnp.float32)

def rope_tables(length, head_width):
    half_width = head_width // 2
    frequency = rope_base ** (-(jnp.arange(half_width, dtype=jnp.float32) * 2.0 / head_width))
    angles = jnp.arange(length, dtype=jnp.float32)[:, None] * frequency[None, :]
    return (jnp.cos(angles)[:, None, :], jnp.sin(angles)[:, None, :])

def rotate(head_rows, cosine, sine_table):
    half_width = head_rows.shape[-1] // 2
    leading = head_rows[..., :half_width]
    trailing = head_rows[..., half_width:]
    return jnp.concatenate([leading * cosine - trailing * sine_table, trailing * cosine + leading * sine_table], axis=-1)

def attend_one(query_rot, key_rot, value_heads, segment_row):
    length = query_rot.shape[0]
    positions = jnp.arange(length)
    allowed = (segment_row[:, None] == segment_row[None, :]) & (positions[None, :] <= positions[:, None])
    score_scale = 1.0 / math.sqrt(HEAD_DIM)
    raw_scores = jnp.einsum('qhgd,khd->hgqk', query_rot, key_rot, precision=lax.Precision.HIGHEST)
    scores = low_back(jnp.where(allowed, raw_scores * score_scale, masked_score))
    row_max = lax.optimization_barrier(jnp.max(scores, axis=-1, keepdims=True))
    expo_rows = jnp.exp(scores - row_max)
    attention = low(expo_rows / lax.optimization_barrier(jnp.sum(expo_rows, axis=-1, keepdims=True)))
    combined = jnp.einsum('hgqk,khd->qhgd', attention, value_heads, precision=lax.Precision.HIGHEST)
    return combined.reshape(length, HEADS * HEAD_DIM)

def layer(params, inputs, segment_rows, cosine, sine_table):
    gains_f, query_w, key_w, value_w, out_w, gate_w, up_w, down_w = params
    group_count, length, model_width = inputs.shape
    residual_in = inputs.reshape(group_count * length, model_width)
    normed_one = residual_in * lax.rsqrt(lax.optimization_barrier(jnp.mean(residual_in * residual_in, axis=-1, keepdims=True)) + eps_norm)
    entry_one = low(normed_one * gains_f[0])
    query_pre = low_back(mixed(entry_one, query_w))
    key_pre = low_back(mixed(entry_one, key_w))
    values = low(low_back(mixed(entry_one, value_w)))
    query_rot = low(rotate(query_pre.reshape(group_count, length, HEADS, HEAD_DIM), cosine, sine_table))
    key_rot = low(rotate(key_pre.reshape(group_count, length, KV_HEADS, HEAD_DIM), cosine, sine_table))
    query_rot = query_rot.reshape(group_count, length, KV_HEADS, HEADS // KV_HEADS, HEAD_DIM)
    value_heads = values.reshape(group_count, length, KV_HEADS, HEAD_DIM)
    checked = jax.checkpoint(attend_one)
    attended = lax.map(lambda group_pack: checked(group_pack[0], group_pack[1], group_pack[2], group_pack[3]), (query_rot, key_rot, value_heads, segment_rows))
    attn_low = low(low_back(attended.reshape(group_count * length, model_width)))
    hidden = residual_in + low_back(mixed(attn_low, out_w))
    normed_two = hidden * lax.rsqrt(lax.optimization_barrier(jnp.mean(hidden * hidden, axis=-1, keepdims=True)) + eps_norm)
    entry_two = low(normed_two * gains_f[1])
    gate_pre = low_back(mixed(entry_two, gate_w))
    up_pre = low_back(mixed(entry_two, up_w))
    act_low = low(gate_pre * jax.nn.sigmoid(gate_pre) * up_pre)
    down_out = low_back(mixed(act_low, down_w))
    return (hidden + down_out).reshape(group_count, length, model_width)

def newton(matrix_low):
    flipped = matrix_low.shape[0] > matrix_low.shape[1]
    oriented = matrix_low.T if flipped else matrix_low
    as_float = oriented.astype(jnp.float32)
    frobenius = jnp.sqrt(jnp.sum(as_float * as_float))
    iterate = (as_float / (frobenius + 1e-07)).astype(jnp.bfloat16)
    for number in range(NS_STEPS):
        gram_low = jnp.dot(iterate, iterate.T, preferred_element_type=jnp.float32).astype(jnp.bfloat16)
        square = jnp.dot(gram_low, gram_low, preferred_element_type=jnp.float32)
        mixer = (coeff_b * gram_low.astype(jnp.float32) + coeff_c * square).astype(jnp.bfloat16)
        product = jnp.dot(mixer, iterate, preferred_element_type=jnp.float32)
        iterate = (coeff_a * iterate.astype(jnp.float32) + product).astype(jnp.bfloat16)
    result = iterate.T if flipped else iterate
    return result

def reference(tokens, segments, cotangent, norm_gains, w_query, w_key, w_value, w_out, w_gate, w_up, w_down, moment_gains, moment_query, moment_key, moment_value, moment_out, moment_gate, moment_up, moment_down):
    params = tuple((weight.astype(jnp.float32) for weight in (norm_gains, w_query, w_key, w_value, w_out, w_gate, w_up, w_down)))
    group_size = math.gcd(NSEQ, max(1, 4096 // SEQ_LEN))
    group_total = NSEQ // group_size
    cosine, sine_table = rope_tables(SEQ_LEN, HEAD_DIM)
    inputs_all = tokens.astype(jnp.float32).reshape(group_total, group_size, SEQ_LEN, D)
    segment_all = segments.reshape(group_total, group_size, SEQ_LEN)
    cot_all = cotangent.astype(jnp.float32).reshape(group_total, group_size, SEQ_LEN, D)

    def one_group(totals, group_pack):
        inputs, segment_rows, cot_rows = group_pack
        output, pullback = jax.vjp(lambda weights, activations: layer(weights, activations, segment_rows, cosine, sine_table), params, inputs)
        grad_params, grad_inputs = pullback(cot_rows)
        totals = tuple((running + addition for running, addition in zip(totals, grad_params)))
        return (totals, (output.astype(jnp.bfloat16), grad_inputs))
    zero_grads = tuple((jnp.zeros_like(weight) for weight in params))
    grad_list, (output_all, grad_all) = lax.scan(one_group, zero_grads, (inputs_all, segment_all, cot_all))
    outputs = output_all.reshape(TOKENS, D)
    grad_tokens = grad_all.reshape(TOKENS, D)
    moments_old = (moment_gains, moment_query, moment_key, moment_value, moment_out, moment_gate, moment_up, moment_down)
    new_moments = tuple((beta_moment * old_moment + grad_full for old_moment, grad_full in zip(moments_old, grad_list)))
    nesterov = tuple(((grad_full + beta_moment * moment_now).astype(jnp.bfloat16) for grad_full, moment_now in zip(grad_list, new_moments)))
    gain_dir = nesterov[0].astype(jnp.float32)
    update_gains = -rate_gain * gain_dir * lax.rsqrt(lax.optimization_barrier(jnp.mean(gain_dir * gain_dir, axis=-1, keepdims=True)) + 1e-06)
    updates = [update_gains]
    for index_id in range(1, 8):
        matrix_low = nesterov[index_id]
        row_count, col_count = matrix_low.shape
        factor = math.sqrt(max(1.0, col_count / row_count))
        updates.append(-rate_matrix * factor * newton(matrix_low).astype(jnp.float32))
    return (outputs, grad_tokens, grad_list[0], grad_list[1], grad_list[2], grad_list[3], grad_list[4], grad_list[5], grad_list[6], grad_list[7], updates[0], updates[1], updates[2], updates[3], updates[4], updates[5], updates[6], updates[7], new_moments[0], new_moments[1], new_moments[2], new_moments[3], new_moments[4], new_moments[5], new_moments[6], new_moments[7])
```

```python
import functools
import math

import jax
import jax.numpy as jnp
from jax import lax
from jax.experimental import pallas as pl
from jax.experimental.pallas import tpu as pltpu
from jax.sharding import PartitionSpec as P

D = 1536
HEADS = 16
KV_HEADS = 8
HEAD_DIM = 96
FF = 4096
KVW = 768

eps_norm = 1e-05
rope_base = 100000.0
coeff_a = 3.4445
coeff_b = -4.775
coeff_c = 2.0315
beta_moment = 0.95
rate_matrix = 0.2
rate_gain = 0.05
masked_score = -1e30

MESH = pl.DeviceIdType.MESH
low_type = jnp.bfloat16
wide_type = jnp.float32


class Place:
    def __init__(self, dp, fs):
        self.dp, self.fs, self.nd = dp, fs, dp * fs
        self.z = lax.axis_index("dp")
        self.f = lax.axis_index("fsdp")
        self.me = self.z * fs + self.f

    def of(self, index):
        return (index // self.fs, lax.rem(index, self.fs))


class Op:
    def __init__(self, source):
        self.source = source

    def scratch(self):
        return [
            pltpu.SemaphoreType.DMA,
            pltpu.SemaphoreType.DMA,
            pltpu.SemaphoreType.DMA,
            pltpu.VMEM(self.block_shape(), self.source.dtype),
        ]

    def block_shape(self):
        return self.source.shape[1:]

    def send(self, at, target):
        src, dst, (send_sem, recv_sem, _, _) = at
        return src, dst, send_sem, recv_sem

    def keep(self, at, src_block, dst_block):
        _, _, (_, _, own_sem, own) = at
        copy = pltpu.make_async_copy(src_block, own, own_sem)
        copy.start()
        copy.wait()
        copy = pltpu.make_async_copy(own, dst_block, own_sem)
        copy.start()
        copy.wait()

    def push(self, at, src_block, dst_block, device):
        _, _, (send_sem, recv_sem, _, _) = at
        pltpu.make_async_remote_copy(
            src_block, dst_block, send_sem, recv_sem, device_id=device, device_id_type=MESH
        ).start()

    def settle(self, at, sent, received):
        _, dst, (send_sem, recv_sem, _, _) = at
        if sent:
            part = dst.at[pl.ds(0, sent)]
            pltpu.make_async_copy(part, part, send_sem).wait()
        if received:
            part = dst.at[pl.ds(0, received)]
            pltpu.make_async_copy(part, part, recv_sem).wait()


class AllToAll(Op):
    def out(self, dp, fs):
        return jax.ShapeDtypeStruct((dp * fs,) + self.source.shape[1:], self.source.dtype)

    def pick(self, place, src, index):
        if self.source.shape[0] == place.nd:
            return src.at[index]
        return src.at[lax.rem(index, place.fs)]

    def start(self, place, at):
        src, dst, _ = at

        def step(k, carry):
            target = lax.rem(place.me + k, place.nd)
            self.push(at, self.pick(place, src, target), dst.at[place.me], place.of(target))
            return carry

        lax.fori_loop(1, place.nd, step, 0)
        self.keep(at, self.pick(place, src, place.me), dst.at[place.me])

    def finish(self, place, at):
        self.settle(at, place.nd - 1, place.nd - 1)


class SpreadAll(AllToAll):
    def block_shape(self):
        return self.source.shape

    def out(self, dp, fs):
        return jax.ShapeDtypeStruct((dp * fs,) + self.source.shape, self.source.dtype)

    def pick(self, place, src, index):
        return src


class PlaneAllToAll(Op):
    def out(self, dp, fs):
        return jax.ShapeDtypeStruct((fs,) + self.source.shape[1:], self.source.dtype)

    def pick(self, src, index):
        return src.at[index]

    def start(self, place, at):
        src, dst, _ = at

        def step(k, carry):
            target = lax.rem(place.f + k, place.fs)
            self.push(at, self.pick(src, target), dst.at[place.f], (place.z, target))
            return carry

        lax.fori_loop(1, place.fs, step, 0)
        self.keep(at, self.pick(src, place.f), dst.at[place.f])

    def finish(self, place, at):
        self.settle(at, place.fs - 1, place.fs - 1)


class PlaneSpread(PlaneAllToAll):
    def block_shape(self):
        return self.source.shape

    def out(self, dp, fs):
        return jax.ShapeDtypeStruct((fs,) + self.source.shape, self.source.dtype)

    def scratch(self):
        half = self.source_half
        return [
            pltpu.SemaphoreType.DMA,
            pltpu.SemaphoreType.DMA((half,)),
            pltpu.SemaphoreType.DMA,
            pltpu.VMEM(self.block_shape(), self.source.dtype),
            pltpu.SemaphoreType.DMA,
            pltpu.SemaphoreType.DMA,
        ]

    def __init__(self, source, fs):
        super().__init__(source)
        self.source_half = fs // 2

    def start(self, place, at):
        src, dst, (send_sem, recv_sems, own_sem, own, pair_send, pair_recv) = at
        core = lax.rem(place.f, 2)
        chip = place.f // 2
        half = place.fs // 2
        for k in range(1, half):
            target = lax.rem(chip + k, half)
            pltpu.make_async_remote_copy(
                src,
                dst.at[place.f],
                send_sem,
                recv_sems.at[k],
                device_id=(place.z, 2 * target + core),
                device_id_type=MESH,
            ).start()
        pltpu.make_async_remote_copy(
            src,
            dst.at[place.f],
            pair_send,
            pair_recv,
            device_id=(place.z, 2 * chip + 1 - core),
            device_id_type=MESH,
        ).start()
        copy = pltpu.make_async_copy(src, own, own_sem)
        copy.start()
        copy.wait()
        copy = pltpu.make_async_copy(own, dst.at[place.f], own_sem)
        copy.start()
        copy.wait()

    def finish(self, place, at):
        src, dst, (send_sem, recv_sems, own_sem, own, pair_send, pair_recv) = at
        core = lax.rem(place.f, 2)
        chip = place.f // 2
        half = place.fs // 2
        for k in range(1, half):
            origin = 2 * lax.rem(chip + half - k, half) + core
            block = dst.at[origin]
            pltpu.make_async_copy(block, block, recv_sems.at[k]).wait()
            pltpu.make_async_remote_copy(
                block,
                block,
                pair_send,
                pair_recv,
                device_id=(place.z, 2 * chip + 1 - core),
                device_id_type=MESH,
            ).start()
        if half > 1:
            part = dst.at[pl.ds(0, half - 1)]
            pltpu.make_async_copy(part, part, send_sem).wait()
        part = dst.at[pl.ds(0, half)]
        pltpu.make_async_copy(part, part, pair_send).wait()
        pltpu.make_async_copy(part, part, pair_recv).wait()


class ChainAllToAll(Op):
    def out(self, dp, fs):
        return jax.ShapeDtypeStruct((dp,) + self.source.shape[1:], self.source.dtype)

    def pick(self, src, index):
        return src.at[index]

    def start(self, place, at):
        src, dst, _ = at

        def step(k, carry):
            target = lax.rem(place.z + k, place.dp)
            self.push(at, self.pick(src, target), dst.at[place.z], (target, place.f))
            return carry

        lax.fori_loop(1, place.dp, step, 0)
        self.keep(at, self.pick(src, place.z), dst.at[place.z])

    def finish(self, place, at):
        self.settle(at, place.dp - 1, place.dp - 1)


class ChainSpread(ChainAllToAll):
    def block_shape(self):
        return self.source.shape

    def out(self, dp, fs):
        return jax.ShapeDtypeStruct((dp,) + self.source.shape, self.source.dtype)

    def pick(self, src, index):
        return src


class OutRows(Op):
    def block_shape(self):
        return self.source.shape

    def out(self, dp, fs):
        return jax.ShapeDtypeStruct((dp,) + self.source.shape, self.source.dtype)

    def start(self, place, at):
        src, dst, _ = at
        column, slot = place.me // place.dp, lax.rem(place.me, place.dp)
        for q in range(place.dp):
            own = (place.z == q) & (place.f == column)

            @pl.when(own)
            def _():
                self.keep(at, src, dst.at[slot])

            @pl.when(jnp.logical_not(own))
            def _():
                self.push(at, src, dst.at[slot], (q, column))

    def finish(self, place, at):
        mine = place.me // place.dp == place.f

        @pl.when(mine)
        def _():
            self.settle(at, place.dp - 1, place.dp - 1)

        @pl.when(jnp.logical_not(mine))
        def _():
            self.settle(at, place.dp, place.dp)


class OutGrads(Op):
    def out(self, dp, fs):
        return jax.ShapeDtypeStruct((dp,) + self.source.shape[1:], self.source.dtype)

    def start(self, place, at):
        src, dst, _ = at
        for i in range(place.dp):
            owner = place.f * place.dp + i

            @pl.when(owner == place.me)
            def _():
                self.keep(at, src.at[i], dst.at[place.z])

            @pl.when(owner != place.me)
            def _():
                self.push(at, src.at[i], dst.at[place.z], place.of(owner))

    def finish(self, place, at):
        mine = place.me // place.dp == place.f

        @pl.when(mine)
        def _():
            self.settle(at, place.dp - 1, place.dp - 1)

        @pl.when(jnp.logical_not(mine))
        def _():
            self.settle(at, place.dp, place.dp)


class ToOwners(Op):
    def __init__(self, source, owner_ids):
        super().__init__(source)
        self.owner_ids = owner_ids

    def out(self, dp, fs):
        return jax.ShapeDtypeStruct((dp * fs,) + self.source.shape[1:], self.source.dtype)

    def start(self, place, at):
        src, dst, _ = at
        for i, owner in enumerate(self.owner_ids):

            @pl.when(place.me != owner)
            def _():
                self.push(at, src.at[i], dst.at[place.me], (owner // place.fs, owner % place.fs))

        for i, owner in enumerate(self.owner_ids):

            @pl.when(place.me == owner)
            def _():
                self.keep(at, src.at[i], dst.at[place.me])

    def finish(self, place, at):
        count = len(self.owner_ids)
        owns = functools.reduce(lambda x, y: x | y, [place.me == o for o in self.owner_ids])

        @pl.when(owns)
        def _():
            self.settle(at, count - 1, place.nd - 1)

        @pl.when(jnp.logical_not(owns))
        def _():
            self.settle(at, count, 0)


class FromOwners(Op):
    def __init__(self, source, owner_ids):
        super().__init__(source)
        self.owner_ids = owner_ids

    def out(self, dp, fs):
        return jax.ShapeDtypeStruct((len(self.owner_ids),) + self.source.shape[1:], self.source.dtype)

    def start(self, place, at):
        src, dst, _ = at
        for i, owner in enumerate(self.owner_ids):

            @pl.when(place.me == owner)
            def _():
                def step(k, carry):
                    target = lax.rem(place.me + k, place.nd)
                    self.push(at, src.at[target], dst.at[i], place.of(target))
                    return carry

                lax.fori_loop(1, place.nd, step, 0)
                self.keep(at, src.at[place.me], dst.at[i])

    def finish(self, place, at):
        _, dst, (send_sem, recv_sem, _, _) = at
        src = at[0]
        count = len(self.owner_ids)
        owns = functools.reduce(lambda x, y: x | y, [place.me == o for o in self.owner_ids])

        @pl.when(owns)
        def _():
            part = src.at[pl.ds(0, place.nd - 1)]
            pltpu.make_async_copy(part, part, send_sem).wait()
            if count > 1:
                part = dst.at[pl.ds(0, count - 1)]
                pltpu.make_async_copy(part, part, recv_sem).wait()

        @pl.when(jnp.logical_not(owns))
        def _():
            part = dst.at[pl.ds(0, count)]
            pltpu.make_async_copy(part, part, recv_sem).wait()


def move(number, dp, fs, *ops):
    count = len(ops)
    scratch = [op.scratch() for op in ops]
    lengths = [len(part) for part in scratch]

    def kernel(*refs):
        place = Place(dp, fs)
        sources, targets, rest = refs[:count], refs[count : 2 * count], list(refs[2 * count :])
        parts = []
        for i in range(count):
            parts.append((sources[i], targets[i], tuple(rest[: lengths[i]])))
            rest = rest[lengths[i] :]
        barrier = pltpu.get_barrier_semaphore()

        def greet(k, carry):
            pl.semaphore_signal(
                barrier, inc=1, device_id=place.of(lax.rem(place.me + k, place.nd)), device_id_type=MESH
            )
            return carry

        lax.fori_loop(1, place.nd, greet, 0)
        pl.semaphore_wait(barrier, place.nd - 1)
        for op, at in zip(ops, parts):
            op.start(place, at)
        for op, at in zip(ops, parts):
            op.finish(place, at)

    return pl.pallas_call(
        kernel,
        out_shape=tuple(op.out(dp, fs) for op in ops),
        in_specs=[pl.BlockSpec(memory_space=pl.ANY)] * count,
        out_specs=tuple([pl.BlockSpec(memory_space=pl.ANY)] * count),
        scratch_shapes=sum(scratch, []),
        compiler_params=pltpu.CompilerParams(collective_id=number, has_side_effects=True),
        name=f"move_{number}",
    )(*[op.source for op in ops])


def rope_tables(length, head_width):
    half_width = head_width // 2
    frequency = rope_base ** (-(jnp.arange(half_width, dtype=jnp.float32) * 2.0 / head_width))
    angles = jnp.arange(length, dtype=jnp.float32)[:, None] * frequency[None, :]
    return (jnp.cos(angles)[:, None, :], jnp.sin(angles)[:, None, :])


def rotate(head_rows, cosine, sine_table):
    half_width = head_rows.shape[-1] // 2
    leading = head_rows[..., :half_width]
    trailing = head_rows[..., half_width:]
    return jnp.concatenate(
        [leading * cosine - trailing * sine_table, trailing * cosine + leading * sine_table],
        axis=-1,
    )


def unrotate(grad_rows, cosine, sine_table):
    half_width = grad_rows.shape[-1] // 2
    leading = grad_rows[..., :half_width]
    trailing = grad_rows[..., half_width:]
    return jnp.concatenate(
        [leading * cosine + trailing * sine_table, trailing * cosine - leading * sine_table],
        axis=-1,
    )


def rms_inverse(activation):
    return lax.rsqrt(jnp.mean(activation * activation, axis=-1, keepdims=True) + eps_norm)


def rms_back(grad_normed, normed, inverse):
    return inverse * (grad_normed - normed * jnp.mean(grad_normed * normed, axis=-1, keepdims=True))


def mul(left_side, right_side):
    return jnp.dot(left_side, right_side, preferred_element_type=wide_type)


def mul_bt(left_side, right_side):
    return jnp.einsum("ik,jk->ij", left_side, right_side, preferred_element_type=wide_type)


def mul_at(left_side, right_side):
    return jnp.einsum("ki,kj->ij", left_side, right_side, preferred_element_type=wide_type)


def gram_mixer(gram):
    a = coeff_a
    frobenius = jnp.sqrt(jnp.trace(gram))
    scale = 1.0 / (frobenius + 1e-07)
    gram_low = (gram * (scale * scale)).astype(low_type)
    parts = []
    for number in range(3):
        square = mul(gram_low, gram_low)
        part = (coeff_b * gram_low.astype(wide_type) + coeff_c * square).astype(low_type)
        parts.append(part)
        if number < 2:
            half = mul(part, gram_low).astype(low_type)
            gram_low = (
                a * a * gram_low.astype(wide_type)
                + 2.0 * a * half.astype(wide_type)
                + mul(part, half)
            ).astype(low_type)
    first, second, third = parts
    joint = (
        a * (first.astype(wide_type) + second.astype(wide_type)) + mul(second, first)
    ).astype(low_type)
    mixer = a * a * third.astype(wide_type) + a * joint.astype(wide_type) + mul(third, joint)
    return scale, mixer.astype(low_type)


def body(
    tokens,
    segments,
    cotangent,
    norm_gains,
    w_query,
    w_key,
    w_value,
    w_out,
    w_gate,
    w_up,
    w_down,
    moment_gains,
    moment_query,
    moment_key,
    moment_value,
    moment_out,
    moment_gate,
    moment_up,
    moment_down,
):
    dp, fs = lax.axis_size("dp"), lax.axis_size("fsdp")
    nd = dp * fs
    me = lax.axis_index("dp") * fs + lax.axis_index("fsdp")
    place_f = lax.axis_index("fsdp")
    length = tokens.shape[0]
    rows = D // nd
    ff_rows = FF // nd
    ff_part = FF // fs
    q_heads = HEADS // fs
    kv_heads = max(1, KV_HEADS // fs)
    repeat = max(1, fs // KV_HEADS)
    group = q_heads // kv_heads
    q_width, kv_width = q_heads * HEAD_DIM, kv_heads * HEAD_DIM
    go = functools.partial(move, dp=dp, fs=fs)

    def run(number, *ops):
        return move(number, dp, fs, *ops)

    def kv_blocks(weight):
        blocks = weight.reshape(rows, KV_HEADS // kv_heads, kv_width)
        return jnp.repeat(blocks, repeat, axis=1) if repeat > 1 else blocks

    def ff_blocks(weight):
        return (
            weight.reshape(rows, dp, fs, ff_rows).transpose(2, 0, 1, 3).reshape(fs, rows, ff_part)
        )

    qkv_blocks = jnp.concatenate(
        [w_query.reshape(rows, fs, q_width), kv_blocks(w_key), kv_blocks(w_value)], axis=-1
    ).transpose(1, 0, 2)
    qkv_width = q_width + 2 * kv_width

    token_all, segment_all, qkv_all, out_all, gain_all = run(
        0,
        PlaneSpread(tokens, fs),
        PlaneAllToAll(jnp.broadcast_to(segments[None], (fs,) + segments.shape)),
        AllToAll(qkv_blocks),
        OutRows(w_out),
        SpreadAll(norm_gains),
    )
    gain_rows = gain_all.transpose(1, 0, 2).reshape(2, D).astype(wide_type)
    qkv_weight = qkv_all.reshape(D, qkv_width)
    out_weight = out_all.reshape(D // fs, D)

    count = fs * length
    cosine, sine_table = rope_tables(length, HEAD_DIM)
    score_scale = 1.0 / math.sqrt(HEAD_DIM)
    plane_in = token_all.reshape(count, D).astype(wide_type)
    entry_one = (plane_in * rms_inverse(plane_in) * gain_rows[0]).astype(low_type)
    qkv_pre = mul(entry_one, qkv_weight)
    query_rot = rotate(
        qkv_pre[:, :q_width].reshape(fs, length, q_heads, HEAD_DIM), cosine, sine_table
    ).astype(low_type)
    key_rot = rotate(
        qkv_pre[:, q_width : q_width + kv_width].reshape(fs, length, kv_heads, HEAD_DIM),
        cosine,
        sine_table,
    ).astype(low_type)
    values = (
        qkv_pre[:, q_width + kv_width :].reshape(fs, length, kv_heads, HEAD_DIM).astype(low_type)
    )
    query_rot = query_rot.reshape(fs, length, kv_heads, group, HEAD_DIM)
    segment_rows = segment_all.reshape(fs, length)
    positions = jnp.arange(length)
    allowed = (segment_rows[:, :, None] == segment_rows[:, None, :]) & (
        positions[None, None, :] <= positions[None, :, None]
    )
    raw_scores = jnp.einsum(
        "sqhgd,skhd->shgqk", query_rot, key_rot, preferred_element_type=wide_type
    )
    scores = jnp.where(allowed[:, None, None], raw_scores * score_scale, masked_score)
    row_max = jnp.max(scores, axis=-1, keepdims=True)
    expo_rows = jnp.exp(scores - row_max)
    attention = expo_rows / jnp.sum(expo_rows, axis=-1, keepdims=True)
    attention_low = attention.astype(low_type)
    attn_low = (
        jnp.einsum("shgqk,skhd->sqhgd", attention_low, values, preferred_element_type=wide_type)
        .reshape(count, q_width)
        .astype(low_type)
    )
    hidden_part = mul(attn_low, out_weight).astype(low_type).reshape(fs, length, D)

    hidden_all, gate_all = run(1, PlaneAllToAll(hidden_part), AllToAll(ff_blocks(w_gate)))
    residual_in = tokens.astype(wide_type)
    hidden = residual_in + jnp.sum(hidden_all.astype(wide_type), axis=0)
    inverse_two = rms_inverse(hidden)
    normed_two = hidden * inverse_two
    entry_two = (normed_two * gain_rows[1]).astype(low_type)

    entry_all, up_all = run(2, PlaneSpread(entry_two, fs), AllToAll(ff_blocks(w_up)))
    entry_all = entry_all.reshape(count, D)
    gate_weight = gate_all.reshape(D, ff_part)
    up_weight = up_all.reshape(D, ff_part)
    gate_pre = mul(entry_all, gate_weight)
    up_pre = mul(entry_all, up_weight)
    gate_sig = jax.nn.sigmoid(gate_pre)
    act_low = (gate_pre * gate_sig * up_pre).astype(low_type)

    cot_all, down_all = run(3, PlaneSpread(cotangent, fs), ChainSpread(w_down))
    cot_all = cot_all.reshape(count, D)
    down_weight = down_all.reshape(ff_part, D)
    down_part = mul(act_low, down_weight).astype(low_type).reshape(fs, length, D)
    d_act = mul_bt(cot_all, down_weight)
    d_gate_low = (d_act * up_pre * gate_sig * (1.0 + gate_pre * (1.0 - gate_sig))).astype(low_type)
    d_up_low = (d_act * gate_pre * gate_sig).astype(low_type)
    d_entry_part = (mul_bt(d_gate_low, gate_weight) + mul_bt(d_up_low, up_weight)).astype(low_type)
    grad_down_part = mul_at(act_low, cot_all).astype(low_type).reshape(dp, ff_rows, D)
    grad_gate_part = mul_at(entry_all, d_gate_low).astype(low_type).reshape(nd, rows, ff_part)
    grad_up_part = mul_at(entry_all, d_up_low).astype(low_type).reshape(nd, rows, ff_part)

    down_out, d_entry_all, grad_down_all = run(
        4,
        PlaneAllToAll(down_part),
        PlaneAllToAll(d_entry_part.reshape(fs, length, D)),
        ChainAllToAll(grad_down_part),
    )
    outputs = (hidden + jnp.sum(down_out.astype(wide_type), axis=0)).astype(low_type)
    d_entry_two = jnp.sum(d_entry_all.astype(wide_type), axis=0)
    grad_down = jnp.sum(grad_down_all.astype(wide_type), axis=0)
    cot_float = cotangent.astype(wide_type)
    d_hidden = cot_float + rms_back(d_entry_two * gain_rows[1], normed_two, inverse_two)
    d_hidden_low = d_hidden.astype(low_type)

    d_hidden_all, grad_gate_all = run(
        5, PlaneSpread(d_hidden_low, fs), AllToAll(grad_gate_part)
    )
    d_hidden_all = d_hidden_all.reshape(count, D)
    d_attn = mul_bt(d_hidden_all, out_weight).astype(low_type)
    grad_out_part = mul_at(attn_low, d_hidden_all).astype(low_type).reshape(dp, rows, D)
    d_attn = d_attn.reshape(fs, length, kv_heads, group, HEAD_DIM)
    d_probs = jnp.einsum("sqhgd,skhd->shgqk", d_attn, values, preferred_element_type=wide_type)
    d_values = jnp.einsum(
        "shgqk,sqhgd->skhd", attention_low, d_attn, preferred_element_type=wide_type
    )
    row_delta = jnp.sum(attention * d_probs, axis=-1, keepdims=True)
    d_scores = (attention * (d_probs - row_delta)).astype(low_type)
    d_query_rot = (
        jnp.einsum("shgqk,skhd->sqhgd", d_scores, key_rot, preferred_element_type=wide_type)
        * score_scale
    )
    d_key_rot = (
        jnp.einsum("shgqk,sqhgd->skhd", d_scores, query_rot, preferred_element_type=wide_type)
        * score_scale
    )
    d_query = unrotate(d_query_rot.reshape(fs, length, q_heads, HEAD_DIM), cosine, sine_table)
    d_key = unrotate(d_key_rot, cosine, sine_table)
    d_qkv = jnp.concatenate(
        [
            d_query.reshape(count, q_width),
            d_key.reshape(count, kv_width),
            d_values.reshape(count, kv_width),
        ],
        axis=-1,
    ).astype(low_type)
    grad_qkv_part = mul_at(entry_one, d_qkv).astype(low_type).reshape(nd, rows, qkv_width)
    d_first_part = mul_bt(d_qkv, qkv_weight).astype(low_type).reshape(fs, length, D)

    d_first_all, grad_up_all = run(6, PlaneAllToAll(d_first_part), AllToAll(grad_up_part))
    d_entry_one = jnp.sum(d_first_all.astype(wide_type), axis=0)
    inverse_one = rms_inverse(residual_in)
    normed_one = residual_in * inverse_one
    grad_tokens = d_hidden + rms_back(d_entry_one * gain_rows[0], normed_one, inverse_one)
    grad_gain_part = (
        jnp.stack([jnp.sum(d_entry_one * normed_one, axis=0), jnp.sum(d_entry_two * normed_two, axis=0)])
        .reshape(2, nd, rows)
        .transpose(1, 0, 2)
    )

    grad_qkv_all, grad_out_all, grad_gain_all = run(
        7, AllToAll(grad_qkv_part), OutGrads(grad_out_part), AllToAll(grad_gain_part)
    )

    def ff_rows_of(blocks):
        total = jnp.sum(blocks.reshape(dp, fs, rows, ff_part).astype(wide_type), axis=0)
        return total.reshape(fs, rows, dp, ff_rows).transpose(1, 2, 0, 3).reshape(rows, FF)

    qkv_total = jnp.sum(grad_qkv_all.reshape(dp, fs, rows, qkv_width).astype(wide_type), axis=0)
    grad_query = qkv_total[..., :q_width].transpose(1, 0, 2).reshape(rows, D)

    def kv_rows_of(blocks):
        if repeat > 1:
            blocks = jnp.sum(blocks.reshape(fs // repeat, repeat, rows, kv_width), axis=1)
        return blocks.transpose(1, 0, 2).reshape(rows, KVW)

    grad_key = kv_rows_of(qkv_total[..., q_width : q_width + kv_width])
    grad_value = kv_rows_of(qkv_total[..., q_width + kv_width :])
    summed = (
        jnp.sum(grad_gain_all, axis=0),
        grad_query,
        grad_key,
        grad_value,
        jnp.sum(grad_out_all.astype(wide_type), axis=0),
        ff_rows_of(grad_gate_all),
        ff_rows_of(grad_up_all),
        grad_down,
    )
    moments_old = (
        moment_gains,
        moment_query,
        moment_key,
        moment_value,
        moment_out,
        moment_gate,
        moment_up,
        moment_down,
    )
    new_moments = tuple(beta_moment * old + grad for old, grad in zip(moments_old, summed))
    nesterov = tuple(
        (grad + beta_moment * now).astype(low_type) for grad, now in zip(summed, new_moments)
    )

    def linear(z_at, f_at):
        return (z_at % dp) * fs + f_at % fs

    gate_owner, up_owner = linear(1, 0), linear(1, fs - 2)
    down_owner = linear(2, 2)
    query_owner, out_owner = linear(2, 4), linear(0, fs - 2)
    key_owner, value_owner = linear(3, 0), linear(3, 4)
    gain_whole, wide_all, tall_all, square_all, small_all = run(
        8,
        SpreadAll(nesterov[0]),
        ToOwners(jnp.stack([nesterov[5], nesterov[6]]), (gate_owner, up_owner)),
        ToOwners(nesterov[7][None], (down_owner,)),
        ToOwners(jnp.stack([nesterov[1], nesterov[4]]), (query_owner, out_owner)),
        ToOwners(jnp.stack([nesterov[2], nesterov[3]]), (key_owner, value_owner)),
    )
    role = jnp.where(
        (me == gate_owner) | (me == up_owner),
        1,
        jnp.where(
            me == down_owner,
            2,
            jnp.where(
                (me == query_owner) | (me == out_owner),
                3,
                jnp.where((me == key_owner) | (me == value_owner), 4, 0),
            ),
        ),
    )

    def idle_work(wide, tall, square, small):
        return wide, tall, square, small

    def step_rows(block, scale, mixer):
        return (
            coeff_a**3 * scale * block.astype(wide_type) + scale * mul(block, mixer)
        ).astype(low_type)

    def wide_work(wide, tall, square, small):
        matrix = wide.reshape(D, FF)
        scale, mixer = gram_mixer(mul_bt(matrix, matrix))
        result = coeff_a**3 * scale * matrix.astype(wide_type) + scale * mul(mixer, matrix)
        return result.astype(low_type).reshape(wide.shape), tall, square, small

    def rows_work(slot, width):
        def work(*blocks):
            blocks = list(blocks)
            matrix = blocks[slot].reshape(-1, width)
            scale, mixer = gram_mixer(mul_at(matrix, matrix))
            blocks[slot] = step_rows(matrix, scale, mixer).reshape(blocks[slot].shape)
            return tuple(blocks)

        return work

    wide_all, tall_all, square_all, small_all = lax.switch(
        role,
        [idle_work, wide_work, rows_work(1, D), rows_work(2, D), rows_work(3, KVW)],
        wide_all,
        tall_all,
        square_all,
        small_all,
    )
    wide_new, tall_new, square_new, small_new = run(
        9,
        FromOwners(wide_all, (gate_owner, up_owner)),
        FromOwners(tall_all, (down_owner,)),
        FromOwners(square_all, (query_owner, out_owner)),
        FromOwners(small_all, (key_owner, value_owner)),
    )
    gain_dir = gain_whole.transpose(1, 0, 2).reshape(2, D).astype(wide_type)
    gain_scale = lax.rsqrt(jnp.mean(gain_dir * gain_dir, axis=-1, keepdims=True) + 1e-06)
    updates = [-rate_gain * nesterov[0].astype(wide_type) * gain_scale]
    pieces = (
        (square_new[0], D, D),
        (small_new[0], D, KVW),
        (small_new[1], D, KVW),
        (square_new[1], D, D),
        (wide_new[0], D, FF),
        (wide_new[1], D, FF),
        (tall_new[0], FF, D),
    )
    for piece, row_count, col_count in pieces:
        factor = math.sqrt(max(1.0, col_count / row_count))
        updates.append(-rate_matrix * factor * piece.astype(wide_type))
    return (outputs, grad_tokens) + summed + tuple(updates) + new_moments


def solution(mesh):
    by_rows = P(("dp", "fsdp"), None)
    by_columns = P(None, ("dp", "fsdp"))
    per_parameter = (by_columns,) + (by_rows,) * 7
    return jax.shard_map(
        body,
        mesh=mesh,
        in_specs=(by_rows,) * 3 + per_parameter * 2,
        out_specs=(by_rows,) * 2 + per_parameter * 3,
        check_vma=False,
    )
```

```python
import functools
import math

import jax
import jax.numpy as jnp
from jax import lax
from jax.experimental import pallas as pl
from jax.experimental.pallas import tpu as pltpu
from jax.sharding import PartitionSpec as P

D = 1536
HEADS = 16
KV_HEADS = 8
HEAD_DIM = 96
FF = 4096
KVW = 768

eps_norm = 1e-05
rope_base = 100000.0
coeff_a = 3.4445
coeff_b = -4.775
coeff_c = 2.0315
beta_moment = 0.95
rate_matrix = 0.2
rate_gain = 0.05
masked_score = -1e30

MESH = pl.DeviceIdType.MESH
low_type = jnp.bfloat16
wide_type = jnp.float32

TILE = 256
SIDE = D // TILE
TILE_PAIRS = tuple((i, j) for j in range(SIDE) for i in range(j + 1))
ATTENTION_PLANE = 3


class Place:
    def __init__(self, dp, fs):
        self.dp, self.fs, self.nd = dp, fs, dp * fs
        self.z = lax.axis_index("dp")
        self.f = lax.axis_index("fsdp")
        self.me = self.z * fs + self.f

    def of(self, index):
        return (index // self.fs, lax.rem(index, self.fs))


class Op:
    def __init__(self, source):
        self.source = source

    def scratch(self):
        return [
            pltpu.SemaphoreType.DMA,
            pltpu.SemaphoreType.DMA,
            pltpu.SemaphoreType.DMA,
            pltpu.VMEM(self.block_shape(), self.source.dtype),
        ]

    def block_shape(self):
        return self.source.shape[1:]

    def send(self, at, target):
        src, dst, (send_sem, recv_sem, _, _) = at
        return src, dst, send_sem, recv_sem

    def keep(self, at, src_block, dst_block):
        _, _, (_, _, own_sem, own) = at
        copy = pltpu.make_async_copy(src_block, own, own_sem)
        copy.start()
        copy.wait()
        copy = pltpu.make_async_copy(own, dst_block, own_sem)
        copy.start()
        copy.wait()

    def push(self, at, src_block, dst_block, device):
        _, _, (send_sem, recv_sem, _, _) = at
        pltpu.make_async_remote_copy(
            src_block, dst_block, send_sem, recv_sem, device_id=device, device_id_type=MESH
        ).start()

    def settle(self, at, sent, received):
        _, dst, (send_sem, recv_sem, _, _) = at
        if sent:
            part = dst.at[pl.ds(0, sent)]
            pltpu.make_async_copy(part, part, send_sem).wait()
        if received:
            part = dst.at[pl.ds(0, received)]
            pltpu.make_async_copy(part, part, recv_sem).wait()


class AllToAll(Op):
    def out(self, dp, fs):
        return jax.ShapeDtypeStruct((dp * fs,) + self.source.shape[1:], self.source.dtype)

    def pick(self, place, src, index):
        if self.source.shape[0] == place.nd:
            return src.at[index]
        return src.at[lax.rem(index, place.fs)]

    def start(self, place, at):
        src, dst, _ = at

        def step(k, carry):
            target = lax.rem(place.me + k, place.nd)
            self.push(at, self.pick(place, src, target), dst.at[place.me], place.of(target))
            return carry

        lax.fori_loop(1, place.nd, step, 0)
        self.keep(at, self.pick(place, src, place.me), dst.at[place.me])

    def finish(self, place, at):
        self.settle(at, place.nd - 1, place.nd - 1)


class SpreadAll(AllToAll):
    def block_shape(self):
        return self.source.shape

    def out(self, dp, fs):
        return jax.ShapeDtypeStruct((dp * fs,) + self.source.shape, self.source.dtype)

    def pick(self, place, src, index):
        return src


class PlaneAllToAll(Op):
    def out(self, dp, fs):
        return jax.ShapeDtypeStruct((fs,) + self.source.shape[1:], self.source.dtype)

    def pick(self, src, index):
        return src.at[index]

    def start(self, place, at):
        src, dst, _ = at

        def step(k, carry):
            target = lax.rem(place.f + k, place.fs)
            self.push(at, self.pick(src, target), dst.at[place.f], (place.z, target))
            return carry

        lax.fori_loop(1, place.fs, step, 0)
        self.keep(at, self.pick(src, place.f), dst.at[place.f])

    def finish(self, place, at):
        self.settle(at, place.fs - 1, place.fs - 1)


class PlaneSpread(PlaneAllToAll):
    def block_shape(self):
        return self.source.shape

    def out(self, dp, fs):
        return jax.ShapeDtypeStruct((fs,) + self.source.shape, self.source.dtype)

    def scratch(self):
        half = self.source_half
        return [
            pltpu.SemaphoreType.DMA,
            pltpu.SemaphoreType.DMA((half,)),
            pltpu.SemaphoreType.DMA,
            pltpu.VMEM(self.block_shape(), self.source.dtype),
            pltpu.SemaphoreType.DMA,
            pltpu.SemaphoreType.DMA,
        ]

    def __init__(self, source, fs):
        super().__init__(source)
        self.source_half = fs // 2

    def start(self, place, at):
        src, dst, (send_sem, recv_sems, own_sem, own, pair_send, pair_recv) = at
        core = lax.rem(place.f, 2)
        chip = place.f // 2
        half = place.fs // 2
        for k in range(1, half):
            target = lax.rem(chip + k, half)
            pltpu.make_async_remote_copy(
                src,
                dst.at[place.f],
                send_sem,
                recv_sems.at[k],
                device_id=(place.z, 2 * target + core),
                device_id_type=MESH,
            ).start()
        pltpu.make_async_remote_copy(
            src,
            dst.at[place.f],
            pair_send,
            pair_recv,
            device_id=(place.z, 2 * chip + 1 - core),
            device_id_type=MESH,
        ).start()
        copy = pltpu.make_async_copy(src, own, own_sem)
        copy.start()
        copy.wait()
        copy = pltpu.make_async_copy(own, dst.at[place.f], own_sem)
        copy.start()
        copy.wait()

    def finish(self, place, at):
        src, dst, (send_sem, recv_sems, own_sem, own, pair_send, pair_recv) = at
        core = lax.rem(place.f, 2)
        chip = place.f // 2
        half = place.fs // 2
        for k in range(1, half):
            origin = 2 * lax.rem(chip + half - k, half) + core
            block = dst.at[origin]
            pltpu.make_async_copy(block, block, recv_sems.at[k]).wait()
            pltpu.make_async_remote_copy(
                block,
                block,
                pair_send,
                pair_recv,
                device_id=(place.z, 2 * chip + 1 - core),
                device_id_type=MESH,
            ).start()
        if half > 1:
            part = dst.at[pl.ds(0, half - 1)]
            pltpu.make_async_copy(part, part, send_sem).wait()
        part = dst.at[pl.ds(0, half)]
        pltpu.make_async_copy(part, part, pair_send).wait()
        pltpu.make_async_copy(part, part, pair_recv).wait()


class PlaneReduce(Op):
    def __init__(self, source, fs, kind):
        super().__init__(source)
        self.half, self.kind = fs // 2, kind

    def out(self, dp, fs):
        return jax.ShapeDtypeStruct((1,) + self.source.shape[1:], self.kind)

    def scratch(self):
        half, block = self.half, self.source.shape[1:]
        slots = (half,) + block
        return [pltpu.SemaphoreType.DMA((half,))] * 5 + [
            pltpu.VMEM(slots, self.source.dtype),
            pltpu.VMEM(slots, self.source.dtype),
            pltpu.VMEM(slots, self.source.dtype),
            pltpu.VMEM(slots, self.source.dtype),
            pltpu.VMEM(block, self.kind),
        ]

    def chip(self, place, k):
        return (place.f // 2) ^ k, lax.rem(place.f, 2)

    def load(self, place, at, k):
        chip, core = self.chip(place, k)
        return pltpu.make_async_copy(at[0].at[2 * chip + core], at[2][5].at[k], at[2][0].at[k])

    def pair(self, place, at, k):
        chip, core = self.chip(place, k)
        return pltpu.make_async_remote_copy(
            at[0].at[2 * chip + 1 - core],
            at[2][6].at[k],
            at[2][1].at[k],
            at[2][2].at[k],
            device_id=(place.z, place.f + 1 - 2 * core),
            device_id_type=MESH,
        )

    def hop(self, place, at, k):
        chip, core = self.chip(place, k)
        return pltpu.make_async_remote_copy(
            at[2][7].at[k],
            at[2][8].at[k],
            at[2][3].at[k],
            at[2][4].at[k],
            device_id=(place.z, 2 * chip + core),
            device_id_type=MESH,
        )

    def order(self):
        return list(reversed(range(self.half)))

    def start(self, place, at):
        for k in self.order():
            self.pair(place, at, k).start()
            self.load(place, at, k).start()

    def combine(self, place, at):
        mine, got, joint, came, result = at[2][5:10]
        high = self.source.shape[1]
        step_rows = 16
        steps = high // step_rows

        def part(n):
            return pl.ds(pl.multiple_of(n * step_rows, step_rows), step_rows)

        for k in self.order():
            self.load(place, at, k).wait()
            self.pair(place, at, k).wait_recv()
            if k:

                def add(n, carry, k=k):
                    total = mine[k, part(n)].astype(wide_type) + got[k, part(n)].astype(wide_type)
                    joint[k, part(n)] = total.astype(joint.dtype)
                    return carry

                lax.fori_loop(0, steps, add, 0)
                self.hop(place, at, k).start()
        for k in self.order():
            if k:
                self.hop(place, at, k).wait_recv()

        def total_of(n, carry):
            total = mine[0, part(n)].astype(wide_type) + got[0, part(n)].astype(wide_type)
            for k in range(1, self.half):
                total = total + came[k, part(n)].astype(wide_type)
            result[part(n)] = total.astype(result.dtype)
            return carry

        lax.fori_loop(0, steps, total_of, 0)

    def release(self, place, at):
        for k in self.order():
            self.pair(place, at, k).wait_send()
            if k:
                self.hop(place, at, k).wait_send()

    def finish(self, place, at):
        self.combine(place, at)
        write = pltpu.make_async_copy(at[2][9], at[1].at[0], at[2][0].at[0])
        write.start()
        self.release(place, at)
        write.wait()


class PlaneTotal(PlaneReduce):
    def __init__(self, source, fs):
        super().__init__(source, fs, source.dtype)

    def out(self, dp, fs):
        return jax.ShapeDtypeStruct((fs,) + self.source.shape[1:], self.source.dtype)

    def scratch(self):
        return super().scratch() + [
            pltpu.SemaphoreType.DMA((self.half,)),
            pltpu.SemaphoreType.DMA((self.half,)),
            pltpu.SemaphoreType.DMA((self.half,)),
            pltpu.SemaphoreType.DMA((self.half,)),
        ]

    def across(self, place, at, k):
        chip, core = self.chip(place, k)
        return pltpu.make_async_remote_copy(
            at[2][9],
            at[1].at[place.f],
            at[2][10].at[k],
            at[2][11].at[k],
            device_id=(place.z, 2 * chip + core),
            device_id_type=MESH,
        )

    def onward(self, place, at, k):
        chip, core = self.chip(place, k)
        block = at[1].at[2 * chip + core]
        return pltpu.make_async_remote_copy(
            block if k else at[2][9],
            block,
            at[2][12].at[k],
            at[2][13].at[k],
            device_id=(place.z, place.f + 1 - 2 * core),
            device_id_type=MESH,
        )

    def finish(self, place, at):
        self.combine(place, at)
        for k in self.order():
            if k:
                self.across(place, at, k).start()
        self.onward(place, at, 0).start()
        write = pltpu.make_async_copy(at[2][9], at[1].at[place.f], at[2][0].at[0])
        write.start()
        for k in self.order():
            if k:
                self.across(place, at, k).wait_recv()
                self.onward(place, at, k).start()
        self.release(place, at)
        write.wait()
        for k in self.order():
            if k:
                self.across(place, at, k).wait_send()
            self.onward(place, at, k).wait()


class ToPlanes(Op):
    def __init__(self, source, planes):
        super().__init__(source)
        self.planes = planes

    def block_shape(self):
        return self.source.shape[2:]

    def out(self, dp, fs):
        return jax.ShapeDtypeStruct((dp * fs,) + self.source.shape[2:], self.source.dtype)

    def start(self, place, at):
        src, dst, _ = at
        for i, plane in enumerate(self.planes):

            def step(k, carry, i=i, plane=plane):
                target = lax.rem(place.f + k, place.fs)
                self.push(at, src.at[i, target], dst.at[place.me], (plane, target))
                return carry

            lax.fori_loop(1, place.fs, step, 0)

            @pl.when(place.z == plane)
            def _():
                self.keep(at, src.at[i, place.f], dst.at[place.me])

            @pl.when(place.z != plane)
            def _():
                self.push(at, src.at[i, place.f], dst.at[place.me], (plane, place.f))

    def finish(self, place, at):
        total = len(self.planes) * place.fs
        inside = functools.reduce(lambda x, y: x | y, [place.z == p for p in self.planes])

        @pl.when(inside)
        def _():
            self.settle(at, total - 1, place.nd - 1)

        @pl.when(jnp.logical_not(inside))
        def _():
            self.settle(at, total, 0)


class FromPlanes(Op):
    def __init__(self, source, planes):
        super().__init__(source)
        self.planes = planes

    def out(self, dp, fs):
        return jax.ShapeDtypeStruct((len(self.planes) * fs,) + self.source.shape[1:], self.source.dtype)

    def start(self, place, at):
        src, dst, _ = at
        for i, plane in enumerate(self.planes):

            @pl.when(place.z == plane)
            def _():
                slot = i * place.fs + place.f

                def step(k, carry):
                    target = lax.rem(place.me + k, place.nd)
                    self.push(at, src.at[target], dst.at[slot], place.of(target))
                    return carry

                lax.fori_loop(1, place.nd, step, 0)
                self.keep(at, src.at[place.me], dst.at[slot])

    def finish(self, place, at):
        src, dst, (send_sem, recv_sem, _, _) = at
        total = len(self.planes) * place.fs
        inside = functools.reduce(lambda x, y: x | y, [place.z == p for p in self.planes])

        @pl.when(inside)
        def _():
            part = src.at[pl.ds(0, place.nd - 1)]
            pltpu.make_async_copy(part, part, send_sem).wait()
            self.settle(at, 0, total - 1)

        @pl.when(jnp.logical_not(inside))
        def _():
            self.settle(at, 0, total)


class ToPlaneOnly(Op):
    def __init__(self, source, plane):
        super().__init__(source)
        self.plane = plane

    def block_shape(self):
        return self.source.shape

    def out(self, dp, fs):
        return jax.ShapeDtypeStruct((dp,) + self.source.shape, self.source.dtype)

    def start(self, place, at):
        src, dst, _ = at

        @pl.when(place.z == self.plane)
        def _():
            self.keep(at, src, dst.at[place.z])

        @pl.when(place.z != self.plane)
        def _():
            self.push(at, src, dst.at[place.z], (self.plane, place.f))

    def finish(self, place, at):
        @pl.when(place.z == self.plane)
        def _():
            self.settle(at, 0, place.dp - 1)

        @pl.when(place.z != self.plane)
        def _():
            self.settle(at, 1, 0)


class FromPlaneOnly(Op):
    def __init__(self, source, plane):
        super().__init__(source)
        self.plane = plane

    def out(self, dp, fs):
        return jax.ShapeDtypeStruct((1,) + self.source.shape[1:], self.source.dtype)

    def start(self, place, at):
        src, dst, _ = at

        @pl.when(place.z == self.plane)
        def _():
            for q in range(place.dp):
                if q != self.plane:
                    self.push(at, src.at[q], dst.at[0], (q, place.f))
            self.keep(at, src.at[self.plane], dst.at[0])

    def finish(self, place, at):
        src, dst, (send_sem, recv_sem, _, _) = at

        @pl.when(place.z == self.plane)
        def _():
            part = src.at[pl.ds(0, place.dp - 1)]
            pltpu.make_async_copy(part, part, send_sem).wait()

        @pl.when(place.z != self.plane)
        def _():
            self.settle(at, 0, 1)


class OutToPlane(Op):
    def out(self, dp, fs):
        return jax.ShapeDtypeStruct((dp,) + self.source.shape[1:], self.source.dtype)

    def start(self, place, at):
        src, dst, _ = at
        for i in range(place.dp):
            owner = place.f * place.dp + i
            slot, target = owner // place.fs, lax.rem(owner, place.fs)

            @pl.when(target == place.f)
            def _():
                self.keep(at, src.at[i], dst.at[slot])

            @pl.when(target != place.f)
            def _():
                self.push(at, src.at[i], dst.at[slot], (place.z, target))

    def finish(self, place, at):
        first = lax.rem(place.f * place.dp, place.fs)
        mine = lax.rem(place.f + place.fs - first, place.fs) < place.dp

        @pl.when(mine)
        def _():
            self.settle(at, place.dp - 1, place.dp - 1)

        @pl.when(jnp.logical_not(mine))
        def _():
            self.settle(at, place.dp, place.dp)


class ChainAllToAll(Op):
    def out(self, dp, fs):
        return jax.ShapeDtypeStruct((dp,) + self.source.shape[1:], self.source.dtype)

    def pick(self, src, index):
        return src.at[index]

    def start(self, place, at):
        src, dst, _ = at

        def step(k, carry):
            target = lax.rem(place.z + k, place.dp)
            self.push(at, self.pick(src, target), dst.at[place.z], (target, place.f))
            return carry

        lax.fori_loop(1, place.dp, step, 0)
        self.keep(at, self.pick(src, place.z), dst.at[place.z])

    def finish(self, place, at):
        self.settle(at, place.dp - 1, place.dp - 1)


class ChainSpread(ChainAllToAll):
    def block_shape(self):
        return self.source.shape

    def out(self, dp, fs):
        return jax.ShapeDtypeStruct((dp,) + self.source.shape, self.source.dtype)

    def pick(self, src, index):
        return src


class OutRows(Op):
    def block_shape(self):
        return self.source.shape

    def out(self, dp, fs):
        return jax.ShapeDtypeStruct((dp,) + self.source.shape, self.source.dtype)

    def start(self, place, at):
        src, dst, _ = at
        column, slot = place.me // place.dp, lax.rem(place.me, place.dp)
        for q in range(place.dp):
            own = (place.z == q) & (place.f == column)

            @pl.when(own)
            def _():
                self.keep(at, src, dst.at[slot])

            @pl.when(jnp.logical_not(own))
            def _():
                self.push(at, src, dst.at[slot], (q, column))

    def finish(self, place, at):
        mine = place.me // place.dp == place.f

        @pl.when(mine)
        def _():
            self.settle(at, place.dp - 1, place.dp - 1)

        @pl.when(jnp.logical_not(mine))
        def _():
            self.settle(at, place.dp, place.dp)


class ToOwners(Op):
    def __init__(self, source, owner_ids):
        super().__init__(source)
        self.owner_ids = owner_ids

    def out(self, dp, fs):
        return jax.ShapeDtypeStruct((dp * fs,) + self.source.shape[1:], self.source.dtype)

    def start(self, place, at):
        src, dst, _ = at
        for i, owner in enumerate(self.owner_ids):

            @pl.when(place.me != owner)
            def _():
                self.push(at, src.at[i], dst.at[place.me], (owner // place.fs, owner % place.fs))

        for i, owner in enumerate(self.owner_ids):

            @pl.when(place.me == owner)
            def _():
                self.keep(at, src.at[i], dst.at[place.me])

    def finish(self, place, at):
        count = len(self.owner_ids)
        owns = functools.reduce(lambda x, y: x | y, [place.me == o for o in self.owner_ids])

        @pl.when(owns)
        def _():
            self.settle(at, count - 1, place.nd - 1)

        @pl.when(jnp.logical_not(owns))
        def _():
            self.settle(at, count, 0)


class FromOwners(Op):
    def __init__(self, source, owner_ids):
        super().__init__(source)
        self.owner_ids = owner_ids

    def out(self, dp, fs):
        return jax.ShapeDtypeStruct((len(self.owner_ids),) + self.source.shape[1:], self.source.dtype)

    def start(self, place, at):
        src, dst, _ = at
        for i, owner in enumerate(self.owner_ids):

            @pl.when(place.me == owner)
            def _():
                def step(k, carry):
                    target = lax.rem(place.me + k, place.nd)
                    self.push(at, src.at[target], dst.at[i], place.of(target))
                    return carry

                lax.fori_loop(1, place.nd, step, 0)
                self.keep(at, src.at[place.me], dst.at[i])

    def finish(self, place, at):
        _, dst, (send_sem, recv_sem, _, _) = at
        src = at[0]
        count = len(self.owner_ids)
        owns = functools.reduce(lambda x, y: x | y, [place.me == o for o in self.owner_ids])

        @pl.when(owns)
        def _():
            part = src.at[pl.ds(0, place.nd - 1)]
            pltpu.make_async_copy(part, part, send_sem).wait()
            if count > 1:
                part = dst.at[pl.ds(0, count - 1)]
                pltpu.make_async_copy(part, part, recv_sem).wait()

        @pl.when(jnp.logical_not(owns))
        def _():
            part = dst.at[pl.ds(0, count)]
            pltpu.make_async_copy(part, part, recv_sem).wait()


def move(number, dp, fs, *ops):
    count = len(ops)
    scratch = [op.scratch() for op in ops]
    lengths = [len(part) for part in scratch]

    def kernel(*refs):
        place = Place(dp, fs)
        sources, targets, rest = refs[:count], refs[count : 2 * count], list(refs[2 * count :])
        parts = []
        for i in range(count):
            parts.append((sources[i], targets[i], tuple(rest[: lengths[i]])))
            rest = rest[lengths[i] :]
        barrier = pltpu.get_barrier_semaphore()

        def greet(k, carry):
            pl.semaphore_signal(
                barrier, inc=1, device_id=place.of(lax.rem(place.me + k, place.nd)), device_id_type=MESH
            )
            return carry

        lax.fori_loop(1, place.nd, greet, 0)
        pl.semaphore_wait(barrier, place.nd - 1)
        for op, at in zip(ops, parts):
            op.start(place, at)
        for op, at in zip(ops, parts):
            op.finish(place, at)

    return pl.pallas_call(
        kernel,
        out_shape=tuple(op.out(dp, fs) for op in ops),
        in_specs=[pl.BlockSpec(memory_space=pl.ANY)] * count,
        out_specs=tuple([pl.BlockSpec(memory_space=pl.ANY)] * count),
        scratch_shapes=sum(scratch, []),
        compiler_params=pltpu.CompilerParams(
            collective_id=number, has_side_effects=True, vmem_limit_bytes=32 << 20
        ),
        name=f"move_{number}",
    )(*[op.source for op in ops])


def rope_tables(length, head_width):
    half_width = head_width // 2
    frequency = rope_base ** (-(jnp.arange(half_width, dtype=jnp.float32) * 2.0 / head_width))
    angles = jnp.arange(length, dtype=jnp.float32)[:, None] * frequency[None, :]
    return (jnp.cos(angles)[:, None, :], jnp.sin(angles)[:, None, :])


def rotate(head_rows, cosine, sine_table):
    half_width = head_rows.shape[-1] // 2
    leading = head_rows[..., :half_width]
    trailing = head_rows[..., half_width:]
    return jnp.concatenate(
        [leading * cosine - trailing * sine_table, trailing * cosine + leading * sine_table],
        axis=-1,
    )


def unrotate(grad_rows, cosine, sine_table):
    half_width = grad_rows.shape[-1] // 2
    leading = grad_rows[..., :half_width]
    trailing = grad_rows[..., half_width:]
    return jnp.concatenate(
        [leading * cosine + trailing * sine_table, trailing * cosine - leading * sine_table],
        axis=-1,
    )


def rms_inverse(activation):
    return lax.rsqrt(jnp.mean(activation * activation, axis=-1, keepdims=True) + eps_norm)


def rms_back(grad_normed, normed, inverse):
    return inverse * (grad_normed - normed * jnp.mean(grad_normed * normed, axis=-1, keepdims=True))


def mul(left_side, right_side):
    return jnp.dot(left_side, right_side, preferred_element_type=wide_type)


def mul_bt(left_side, right_side):
    return jnp.einsum("ik,jk->ij", left_side, right_side, preferred_element_type=wide_type)


def mul_at(left_side, right_side):
    return jnp.einsum("ki,kj->ij", left_side, right_side, preferred_element_type=wide_type)


def mixer_kernel(own_ref, sum_ref, mixer_ref, scale_ref, gram, kept, spare, half):
    a = coeff_a
    alone = lax.axis_index("dp") == ATTENTION_PLANE

    def tile_of(number):
        return jnp.where(alone, own_ref[number], sum_ref[number]).astype(wide_type)

    shape = (TILE, TILE)
    diagonal = lax.broadcasted_iota(jnp.int32, shape, 0) == lax.broadcasted_iota(jnp.int32, shape, 1)
    total = jnp.zeros((1, 1), wide_type)
    for number, (i, j) in enumerate(TILE_PAIRS):
        if i == j:
            kept_part = jnp.where(diagonal, tile_of(number), 0.0)
            total = total + jnp.sum(
                jnp.sum(kept_part, axis=1, keepdims=True), axis=0, keepdims=True
            )
    scale = 1.0 / (jnp.sqrt(total) + 1e-07)
    scale_ref[...] = jnp.broadcast_to(scale, scale_ref.shape)
    square = scale * scale

    def span(i):
        return pl.ds(i * TILE, TILE)

    def put(target, i, j, value):
        target[span(i), span(j)] = value
        if i != j:
            target[span(j), span(i)] = value.T

    for number, (i, j) in enumerate(TILE_PAIRS):
        put(gram, i, j, (tile_of(number) * square).astype(low_type))

    def product(left, right, target, finish):
        for i, j in TILE_PAIRS:
            value = mul(left[span(i), :], right[:, span(j)])
            put(target, i, j, finish(value, lambda ref: ref[span(i), span(j)].astype(wide_type)).astype(low_type))

    def poly(source, target):
        product(
            source, source, target, lambda value, tile: coeff_b * tile(source) + coeff_c * value
        )

    def step(factor, source, target):
        product(factor, source, half, lambda value, tile: value)
        product(
            factor,
            half,
            target,
            lambda value, tile: a * a * tile(source) + 2.0 * a * tile(half) + value,
        )

    poly(gram, kept)
    step(kept, gram, spare)
    poly(spare, gram)
    step(gram, spare, mixer_ref)
    product(gram, kept, half, lambda value, tile: a * (tile(gram) + tile(kept)) + value)
    poly(mixer_ref, spare)
    product(
        spare, half, mixer_ref, lambda value, tile: a * a * tile(spare) + a * tile(half) + value
    )


def gram_mixer(own_tiles, sum_tiles):
    matrix = jax.ShapeDtypeStruct((D, D), low_type)
    mixer, scale = pl.pallas_call(
        mixer_kernel,
        out_shape=(matrix, jax.ShapeDtypeStruct((8, 128), wide_type)),
        in_specs=[pl.BlockSpec(memory_space=pltpu.VMEM)] * 2,
        out_specs=(pl.BlockSpec(memory_space=pltpu.VMEM),) * 2,
        scratch_shapes=[pltpu.VMEM((D, D), low_type)] * 4,
        compiler_params=pltpu.CompilerParams(vmem_limit_bytes=44 << 20),
        name="gram_mixer",
    )(own_tiles, sum_tiles)
    return scale[0, 0], mixer


def body(
    tokens,
    segments,
    cotangent,
    norm_gains,
    w_query,
    w_key,
    w_value,
    w_out,
    w_gate,
    w_up,
    w_down,
    moment_gains,
    moment_query,
    moment_key,
    moment_value,
    moment_out,
    moment_gate,
    moment_up,
    moment_down,
):
    dp, fs = lax.axis_size("dp"), lax.axis_size("fsdp")
    nd = dp * fs
    me = lax.axis_index("dp") * fs + lax.axis_index("fsdp")
    place_f = lax.axis_index("fsdp")
    length = tokens.shape[0]
    rows = D // nd
    ff_rows = FF // nd
    ff_part = FF // fs
    q_heads = HEADS // fs
    kv_heads = max(1, KV_HEADS // fs)
    repeat = max(1, fs // KV_HEADS)
    group = q_heads // kv_heads
    q_width, kv_width = q_heads * HEAD_DIM, kv_heads * HEAD_DIM

    def run(number, *ops):
        return move(number, dp, fs, *ops)

    def kv_blocks(weight):
        blocks = weight.reshape(rows, KV_HEADS // kv_heads, kv_width)
        return jnp.repeat(blocks, repeat, axis=1) if repeat > 1 else blocks

    def ff_blocks(weight):
        return (
            weight.reshape(rows, dp, fs, ff_rows).transpose(2, 0, 1, 3).reshape(fs, rows, ff_part)
        )

    qkv_blocks = jnp.concatenate(
        [w_query.reshape(rows, fs, q_width), kv_blocks(w_key), kv_blocks(w_value)], axis=-1
    ).transpose(1, 0, 2)
    qkv_width = q_width + 2 * kv_width

    token_all, segment_all, qkv_all, out_all, gain_all = run(
        0,
        PlaneSpread(tokens, fs),
        PlaneAllToAll(jnp.broadcast_to(segments[None], (fs,) + segments.shape)),
        AllToAll(qkv_blocks),
        OutRows(w_out),
        SpreadAll(norm_gains),
    )
    gain_rows = gain_all.transpose(1, 0, 2).reshape(2, D).astype(wide_type)
    qkv_weight = qkv_all.reshape(D, qkv_width)
    out_weight = out_all.reshape(D // fs, D)

    count = fs * length
    cosine, sine_table = rope_tables(length, HEAD_DIM)
    score_scale = 1.0 / math.sqrt(HEAD_DIM)
    plane_in = token_all.reshape(count, D).astype(wide_type)
    entry_one = (plane_in * rms_inverse(plane_in) * gain_rows[0]).astype(low_type)
    qkv_pre = mul(entry_one, qkv_weight)
    query_rot = rotate(
        qkv_pre[:, :q_width].reshape(fs, length, q_heads, HEAD_DIM), cosine, sine_table
    ).astype(low_type)
    key_rot = rotate(
        qkv_pre[:, q_width : q_width + kv_width].reshape(fs, length, kv_heads, HEAD_DIM),
        cosine,
        sine_table,
    ).astype(low_type)
    values = (
        qkv_pre[:, q_width + kv_width :].reshape(fs, length, kv_heads, HEAD_DIM).astype(low_type)
    )
    query_rot = query_rot.reshape(fs, length, kv_heads, group, HEAD_DIM)
    segment_rows = segment_all.reshape(fs, length)
    positions = jnp.arange(length)
    allowed = (segment_rows[:, :, None] == segment_rows[:, None, :]) & (
        positions[None, None, :] <= positions[None, :, None]
    )
    raw_scores = jnp.einsum(
        "sqhgd,skhd->shgqk", query_rot, key_rot, preferred_element_type=wide_type
    )
    scores = jnp.where(allowed[:, None, None], raw_scores * score_scale, masked_score)
    row_max = jnp.max(scores, axis=-1, keepdims=True)
    expo_rows = jnp.exp(scores - row_max)
    attention = expo_rows / jnp.sum(expo_rows, axis=-1, keepdims=True)
    attention_low = attention.astype(low_type)
    attn_low = (
        jnp.einsum("shgqk,skhd->sqhgd", attention_low, values, preferred_element_type=wide_type)
        .reshape(count, q_width)
        .astype(low_type)
    )
    hidden_part = mul(attn_low, out_weight).astype(low_type).reshape(fs, length, D)

    hidden_sum, gate_all = run(
        1, PlaneReduce(hidden_part, fs, wide_type), AllToAll(ff_blocks(w_gate))
    )
    residual_in = tokens.astype(wide_type)
    hidden = residual_in + hidden_sum[0]
    inverse_two = rms_inverse(hidden)
    normed_two = hidden * inverse_two
    entry_two = (normed_two * gain_rows[1]).astype(low_type)

    entry_all, up_all = run(2, PlaneSpread(entry_two, fs), AllToAll(ff_blocks(w_up)))
    entry_all = entry_all.reshape(count, D)
    gate_weight = gate_all.reshape(D, ff_part)
    up_weight = up_all.reshape(D, ff_part)
    gate_pre = mul(entry_all, gate_weight)
    up_pre = mul(entry_all, up_weight)
    gate_sig = jax.nn.sigmoid(gate_pre)
    act_low = (gate_pre * gate_sig * up_pre).astype(low_type)

    cot_all, down_all = run(3, PlaneSpread(cotangent, fs), ChainSpread(w_down))
    cot_all = cot_all.reshape(count, D)
    down_weight = down_all.reshape(ff_part, D)
    down_part = mul(act_low, down_weight).astype(low_type).reshape(fs, length, D)
    d_act = mul_bt(cot_all, down_weight)
    d_gate_low = (d_act * up_pre * gate_sig * (1.0 + gate_pre * (1.0 - gate_sig))).astype(low_type)
    d_up_low = (d_act * gate_pre * gate_sig).astype(low_type)
    d_entry_part = (mul_bt(d_gate_low, gate_weight) + mul_bt(d_up_low, up_weight)).astype(low_type)
    grad_down_part = mul_at(act_low, cot_all).astype(low_type).reshape(dp, ff_rows, D)
    grad_gate_part = mul_at(entry_all, d_gate_low).astype(low_type).reshape(nd, rows, ff_part)
    grad_up_part = mul_at(entry_all, d_up_low).astype(low_type).reshape(nd, rows, ff_part)

    down_out, d_entry_all, grad_down_all = run(
        4,
        PlaneReduce(down_part, fs, wide_type),
        PlaneReduce(d_entry_part.reshape(fs, length, D), fs, wide_type),
        ChainAllToAll(grad_down_part),
    )
    outputs = (hidden + down_out[0]).astype(low_type)
    d_entry_two = d_entry_all[0]
    grad_down = jnp.sum(grad_down_all.astype(wide_type), axis=0)
    cot_float = cotangent.astype(wide_type)
    d_hidden = cot_float + rms_back(d_entry_two * gain_rows[1], normed_two, inverse_two)
    d_hidden_low = d_hidden.astype(low_type)

    d_hidden_all, grad_gate_all = run(
        5, PlaneSpread(d_hidden_low, fs), AllToAll(grad_gate_part)
    )
    d_hidden_all = d_hidden_all.reshape(count, D)
    d_attn = mul_bt(d_hidden_all, out_weight).astype(low_type)
    grad_out_part = mul_at(attn_low, d_hidden_all).astype(low_type).reshape(dp, rows, D)
    d_attn = d_attn.reshape(fs, length, kv_heads, group, HEAD_DIM)
    d_probs = jnp.einsum("sqhgd,skhd->shgqk", d_attn, values, preferred_element_type=wide_type)
    d_values = jnp.einsum(
        "shgqk,sqhgd->skhd", attention_low, d_attn, preferred_element_type=wide_type
    )
    row_delta = jnp.sum(attention * d_probs, axis=-1, keepdims=True)
    d_scores = (attention * (d_probs - row_delta)).astype(low_type)
    d_query_rot = (
        jnp.einsum("shgqk,skhd->sqhgd", d_scores, key_rot, preferred_element_type=wide_type)
        * score_scale
    )
    d_key_rot = (
        jnp.einsum("shgqk,sqhgd->skhd", d_scores, query_rot, preferred_element_type=wide_type)
        * score_scale
    )
    d_query = unrotate(d_query_rot.reshape(fs, length, q_heads, HEAD_DIM), cosine, sine_table)
    d_key = unrotate(d_key_rot, cosine, sine_table)
    d_qkv = jnp.concatenate(
        [
            d_query.reshape(count, q_width),
            d_key.reshape(count, kv_width),
            d_values.reshape(count, kv_width),
        ],
        axis=-1,
    ).astype(low_type)
    grad_qkv_part = mul_at(entry_one, d_qkv).astype(low_type).reshape(nd, rows, qkv_width)
    d_first_part = mul_bt(d_qkv, qkv_weight).astype(low_type).reshape(fs, length, D)

    d_first_sum, grad_up_all, grad_out_plane = run(
        6,
        PlaneReduce(d_first_part, fs, wide_type),
        AllToAll(grad_up_part),
        OutToPlane(grad_out_part),
    )
    d_entry_one = d_first_sum[0]
    inverse_one = rms_inverse(residual_in)
    normed_one = residual_in * inverse_one
    grad_tokens = d_hidden + rms_back(d_entry_one * gain_rows[0], normed_one, inverse_one)
    grad_gain_part = (
        jnp.stack([jnp.sum(d_entry_one * normed_one, axis=0), jnp.sum(d_entry_two * normed_two, axis=0)])
        .reshape(2, nd, rows)
        .transpose(1, 0, 2)
    )

    grad_qkv_all, grad_out_all, grad_gain_all = run(
        7, AllToAll(grad_qkv_part), ChainAllToAll(grad_out_plane), AllToAll(grad_gain_part)
    )

    def ff_rows_of(blocks):
        total = jnp.sum(blocks.reshape(dp, fs, rows, ff_part).astype(wide_type), axis=0)
        return total.reshape(fs, rows, dp, ff_rows).transpose(1, 2, 0, 3).reshape(rows, FF)

    qkv_total = jnp.sum(grad_qkv_all.reshape(dp, fs, rows, qkv_width).astype(wide_type), axis=0)
    grad_query = qkv_total[..., :q_width].transpose(1, 0, 2).reshape(rows, D)

    def kv_rows_of(blocks):
        if repeat > 1:
            blocks = jnp.sum(blocks.reshape(fs // repeat, repeat, rows, kv_width), axis=1)
        return blocks.transpose(1, 0, 2).reshape(rows, KVW)

    grad_key = kv_rows_of(qkv_total[..., q_width : q_width + kv_width])
    grad_value = kv_rows_of(qkv_total[..., q_width + kv_width :])
    summed = (
        jnp.sum(grad_gain_all, axis=0),
        grad_query,
        grad_key,
        grad_value,
        jnp.sum(grad_out_all.astype(wide_type), axis=0),
        ff_rows_of(grad_gate_all),
        ff_rows_of(grad_up_all),
        grad_down,
    )
    moments_old = (
        moment_gains,
        moment_query,
        moment_key,
        moment_value,
        moment_out,
        moment_gate,
        moment_up,
        moment_down,
    )
    new_moments = tuple(beta_moment * old + grad for old, grad in zip(moments_old, summed))
    nesterov = tuple(
        (grad + beta_moment * now).astype(low_type) for grad, now in zip(summed, new_moments)
    )

    gate_plane, up_plane, down_plane = 0, 1, 2
    query_owner, out_owner, key_owner, value_owner = [
        ATTENTION_PLANE * fs + n for n in (0, 6, 2, 4)
    ]
    gain_whole, wide_all, tall_all, square_all, small_all = run(
        8,
        SpreadAll(nesterov[0]),
        ToPlanes(jnp.stack([ff_blocks(nesterov[5]), ff_blocks(nesterov[6])]), (gate_plane, up_plane)),
        ToPlaneOnly(nesterov[7], down_plane),
        ToOwners(jnp.stack([nesterov[1], nesterov[4]]), (query_owner, out_owner)),
        ToOwners(jnp.stack([nesterov[2], nesterov[3]]), (key_owner, value_owner)),
    )
    place_z = lax.axis_index("dp")
    role = jnp.where(
        (place_z == gate_plane) | (place_z == up_plane),
        1,
        jnp.where(
            place_z == down_plane,
            2,
            jnp.where(
                (me == query_owner) | (me == out_owner),
                3,
                jnp.where((me == key_owner) | (me == value_owner), 4, 0),
            ),
        ),
    )
    tile_slots = -(-len(TILE_PAIRS) // fs)
    packed = (fs * tile_slots, TILE, TILE)

    def tiles_of(gram):
        side = gram.shape[0] // TILE
        blank = jnp.zeros((TILE, TILE), low_type)
        tiles = [
            gram[i * TILE : (i + 1) * TILE, j * TILE : (j + 1) * TILE].astype(low_type)
            if j < side
            else blank
            for i, j in TILE_PAIRS
        ]
        return jnp.stack(tiles + [blank] * (packed[0] - len(tiles)))

    def gram_of_rows(blocks, width):
        matrix = blocks.reshape(-1, width)
        return tiles_of(mul_at(matrix, matrix))

    def gram_of_columns(blocks):
        matrix = blocks.reshape(D, ff_part)
        return tiles_of(mul_bt(matrix, matrix))

    own_tiles = lax.switch(
        role,
        [
            lambda wide, tall, square, small: jnp.zeros(packed, low_type),
            lambda wide, tall, square, small: gram_of_columns(wide),
            lambda wide, tall, square, small: gram_of_rows(tall, D),
            lambda wide, tall, square, small: gram_of_rows(square, D),
            lambda wide, tall, square, small: gram_of_rows(small, KVW),
        ],
        wide_all,
        tall_all,
        square_all,
        small_all,
    )
    (sum_tiles,) = run(9, PlaneTotal(own_tiles.reshape(fs, tile_slots * TILE, TILE), fs))
    scale, mixer = gram_mixer(own_tiles, sum_tiles.reshape(packed))

    def finished(matrix, product):
        return (scale * (coeff_a**3 * matrix.astype(wide_type) + product)).astype(low_type)

    def columns_work(wide, tall, square, small):
        matrix = wide.reshape(D, ff_part)
        return finished(matrix, mul(mixer, matrix)).reshape(wide.shape), tall, square, small

    def rows_work(slot, width):
        def work(*blocks):
            blocks = list(blocks)
            matrix = blocks[slot].reshape(-1, width)
            product = mul(matrix, mixer[:width, :width])
            blocks[slot] = finished(matrix, product).reshape(blocks[slot].shape)
            return tuple(blocks)

        return work

    wide_all, tall_all, square_all, small_all = lax.switch(
        role,
        [lambda *blocks: blocks, columns_work, rows_work(1, D), rows_work(2, D), rows_work(3, KVW)],
        wide_all,
        tall_all,
        square_all,
        small_all,
    )
    wide_new, tall_new, square_new, small_new = run(
        10,
        FromPlanes(wide_all, (gate_plane, up_plane)),
        FromPlaneOnly(tall_all, down_plane),
        FromOwners(square_all, (query_owner, out_owner)),
        FromOwners(small_all, (key_owner, value_owner)),
    )
    wide_new = wide_new.reshape(2, fs, rows, dp, ff_rows).transpose(0, 2, 3, 1, 4).reshape(2, rows, FF)
    gain_dir = gain_whole.transpose(1, 0, 2).reshape(2, D).astype(wide_type)
    gain_scale = lax.rsqrt(jnp.mean(gain_dir * gain_dir, axis=-1, keepdims=True) + 1e-06)
    updates = [-rate_gain * nesterov[0].astype(wide_type) * gain_scale]
    pieces = (
        (square_new[0], D, D),
        (small_new[0], D, KVW),
        (small_new[1], D, KVW),
        (square_new[1], D, D),
        (wide_new[0], D, FF),
        (wide_new[1], D, FF),
        (tall_new[0], FF, D),
    )
    for piece, row_count, col_count in pieces:
        factor = math.sqrt(max(1.0, col_count / row_count))
        updates.append(-rate_matrix * factor * piece.astype(wide_type))
    return (outputs, grad_tokens) + summed + tuple(updates) + new_moments


def solution(mesh):
    by_rows = P(("dp", "fsdp"), None)
    by_columns = P(None, ("dp", "fsdp"))
    per_parameter = (by_columns,) + (by_rows,) * 7
    return jax.shard_map(
        body,
        mesh=mesh,
        in_specs=(by_rows,) * 3 + per_parameter * 2,
        out_specs=(by_rows,) * 2 + per_parameter * 3,
        check_vma=False,
    )
```
